32 devices in a mesh: gx: 2 (over x), gy: 4 (over z), gz: 4 (over y, core).
Axes of the slice: x: 2, y: 2, z: 4, core: 2. Of those that a mesh axis runs over, the one named last changes fastest.
Arguments:
- tokens: bfloat16 [512, 49, 512], P(('gx', 'gy', 'gz')), may hold values from -6 to 6
- cotangent: bfloat16 [512, 49, 512], P(('gx', 'gy', 'gz')), may hold values from -6 to 6
- regions: int32 [512, 49], P(('gx', 'gy', 'gz')), may hold values from 0 to 3
- rel_index: int32 [49, 49], replicated, may hold values from 0 to 168
- w_qkv: bfloat16 [512, 1536], replicated, may hold values from -0.25 to 0.25
- w_proj: bfloat16 [512, 512], replicated, may hold values from -0.25 to 0.25
- bias_table: float32 [169, 16], replicated, may hold values from -4 to 4
- mom_qkv: float32 [786432], P(('gx', 'gy', 'gz')), may hold values from -0.06 to 0.06
- mom_proj: float32 [262144], P(('gx', 'gy', 'gz')), may hold values from -0.06 to 0.06
- mom_table: float32 [169, 16], replicated, may hold values from -0.06 to 0.06
Outputs:
- new_mom_qkv: float32 [786432], P(('gx', 'gy', 'gz'))
- new_mom_proj: float32 [262144], P(('gx', 'gy', 'gz'))
- new_mom_table: float32 [169, 16], replicated
The draws below stay inside these ranges and needn't reach their ends.
All inputs are finite; a program needn't handle non-finite values.
Results may differ from the reference program's by a relative error of at most 0.015.
Values sent between devices are 32-bit elements; how exact they have to be, the bound alone decides.
A program may use at most 128 MiB of HBM per device.

```python
import jax
import jax.numpy as jnp
from jax import lax

D = 512
HEADS = 16
WIN_TOK = 49
TABLE = 169
WIN_DEV = 16
WINDOWS = 512
N_GX = 2
N_GY = 4
N_GZ = 4


def touch_ends(drawn, own_key, smallest, largest):
    dims = drawn.shape
    index_at = [jax.random.randint(jax.random.fold_in(own_key, axis), (), 0, dims[axis]) for axis in range(len(dims))]
    drawn = drawn.at[tuple(index_at)].set(smallest)
    longest = dims.index(max(dims))
    index_at[longest] = (index_at[longest] + 1) % dims[longest]
    return drawn.at[tuple(index_at)].set(largest)


def block_levels(key, shape, cuts, low, largest):
    def one(dim, shards_of):
        steps = jax.random.uniform(jax.random.fold_in(jax.random.fold_in(key, 6), dim), (shards_of,), jnp.float32, low / len(cuts), largest / len(cuts))
        return jnp.repeat(jnp.exp(steps), shape[dim] // shards_of).reshape((-1,) + (1,) * (len(shape) - dim - 1))

    loudness = one(*cuts[0])
    for cut in cuts[1:]:
        loudness = loudness * one(*cut)
    return loudness


def noise(stream_key, extent, deviation, reach, cuts=(), held_as=jnp.bfloat16):
    drawn = deviation * jax.random.normal(stream_key, extent, jnp.float32)
    if cuts:
        drawn = drawn * block_levels(stream_key, extent, cuts, -0.22, 0.18)
    return jnp.clip(drawn, -reach, reach).astype(held_as)


def setup_inputs(seed: int = 0) -> dict:
    key_list = jax.random.split(jax.random.key(seed), 11)
    return {
        "tokens": noise(key_list[0], (WINDOWS, WIN_TOK, D), 1.0, 6.0, ((0, 32),)),
        "cotangent": noise(key_list[1], (WINDOWS, WIN_TOK, D), 1.0, 6.0, ((0, 32),)),
        "regions": touch_ends(jax.random.randint(key_list[2], (WINDOWS, WIN_TOK), 0, 4), jax.random.fold_in(key_list[2], 1), 0, 3).astype(jnp.int32),
        "rel_index": touch_ends(jax.random.randint(key_list[3], (WIN_TOK, WIN_TOK), 0, 169), jax.random.fold_in(key_list[3], 1), 0, 168).astype(jnp.int32),
        "w_qkv": noise(key_list[4], (D, 3 * D), D ** -0.5, 0.25),
        "w_proj": noise(key_list[5], (D, D), D ** -0.5, 0.25),
        "bias_table": noise(key_list[6], (TABLE, HEADS), 1.0, 4.0, (), jnp.float32),
        "mom_qkv": noise(key_list[7], (3 * D * D,), 0.01, 0.06, ((0, 32),), jnp.float32),
        "mom_proj": noise(key_list[8], (D * D,), 0.01, 0.06, ((0, 32),), jnp.float32),
        "mom_table": noise(key_list[9], (TABLE, HEADS), 0.01, 0.06, (), jnp.float32),
    }


def attend_core(qkv, table, regions, rel_index, heads):
    win, count, width = qkv.shape
    dim = width // 3
    parts = qkv.reshape(win, count, 3, heads, dim // heads).astype(jnp.float32)
    bias = jnp.transpose(table[rel_index], (2, 0, 1))
    scores = jnp.einsum('wihc,wjhc->whij', parts[:, :, 0], parts[:, :, 1]) * (dim // heads) ** (-0.5)
    masked = jnp.where(regions[:, :, None] == regions[:, None, :], 0.0, -100.0).astype(jnp.float32)
    scores = scores + bias[None] + masked[:, None]
    probs = jax.nn.softmax(scores, axis=-1).astype(jnp.bfloat16)
    attended = jnp.einsum('whij,wjhc->wihc', probs.astype(jnp.float32), parts[:, :, 2])
    return attended.astype(jnp.bfloat16).reshape(win, count, dim)

def local_grads(tokens, cotangent, regions, rel_index, w_qkv, w_proj, bias_table, heads):
    win, count, dim = tokens.shape
    flat = tokens.reshape(win * count, dim)
    qkv = jnp.dot(flat, w_qkv, preferred_element_type=jnp.float32).astype(jnp.bfloat16).reshape(win, count, 3 * dim)

    def forward(values, table):
        return attend_core(values, table, regions, rel_index, heads)
    attended, pullback = jax.vjp(forward, qkv, bias_table)
    flat_dy = cotangent.reshape(win * count, dim)
    grad_proj = jnp.dot(attended.reshape(win * count, dim).astype(jnp.float32).T, flat_dy.astype(jnp.float32))
    d_attended = jnp.dot(flat_dy, w_proj.T, preferred_element_type=jnp.float32).astype(jnp.bfloat16)
    d_qkv, grad_table = pullback(d_attended.reshape(win, count, dim))
    grad_qkv = jnp.dot(flat.astype(jnp.float32).T, d_qkv.reshape(win * count, 3 * dim).astype(jnp.float32))
    return (grad_qkv, grad_proj, grad_table)

def reference(tokens, cotangent, regions, rel_index, w_qkv, w_proj, bias_table, mom_qkv, mom_proj, mom_table):
    groups = N_GX * N_GY * N_GZ
    heads = bias_table.shape[1]
    tok_groups = tokens.reshape(groups, WIN_DEV, WIN_TOK, D)
    cot_groups = cotangent.reshape(groups, WIN_DEV, WIN_TOK, D)
    reg_groups = regions.reshape(groups, WIN_DEV, WIN_TOK)

    def step(carry, items):
        g_qkv, g_proj, g_table = local_grads(items[0], items[1], items[2], rel_index, w_qkv, w_proj, bias_table, heads)
        return ((carry[0] + g_qkv, carry[1] + g_proj, carry[2] + g_table), None)
    start = (jnp.zeros(w_qkv.shape, jnp.float32), jnp.zeros(w_proj.shape, jnp.float32), jnp.zeros(bias_table.shape, jnp.float32))
    sums, unused = lax.scan(step, start, (tok_groups, cot_groups, reg_groups))
    scale = 1.0 / (WIN_DEV * groups)
    return (0.9 * mom_qkv + sums[0].reshape(-1) * scale, 0.9 * mom_proj + sums[1].reshape(-1) * scale, 0.9 * mom_table + sums[2] * scale)
```

```python
import functools
import math

import jax
import jax.numpy as jnp
from jax import lax
from jax.experimental import pallas as pl
from jax.experimental.pallas import tpu as pltpu
from jax.sharding import PartitionSpec as P

AXES = ("gx", "gy", "gz")
MESH = pl.DeviceIdType.MESH
F32, BF16 = jnp.float32, jnp.bfloat16
PAD = 64
GROUP = 4
LOG2E = math.log2(math.e)
STEPS = 5
NT = (((1,), (1,)), ((), ()))
TN = (((0,), (0,)), ((), ()))


def dot(a, b, dims=(((1,), (0,)), ((), ()))):
    return lax.dot_general(a, b, dims, preferred_element_type=F32)


def spread(value, lanes, width):
    return jnp.concatenate(
        [jnp.where(lanes // width == h, value, jnp.zeros_like(value)) for h in range(GROUP)], axis=0
    )


def gather_heads(value, lanes, width):
    total = jnp.where(lanes // width == 0, value[:PAD], 0.0)
    for h in range(1, GROUP):
        total = jnp.where(lanes // width == h, value[h * PAD : (h + 1) * PAD], total)
    return total


class Exchange:
    def __init__(self, grad, recvs, send_sem, recv_sem, chunk, where):
        self.grad, self.recvs, self.send_sem, self.recv_sem = grad, recvs, send_sem, recv_sem
        self.chunk, self.where, self.step = chunk, where, 0

    def copy(self, half, step):
        bits, partners = self.where[half]
        src = self.grad.at[(half, *bits[:step], 1 - bits[step])]
        return pltpu.make_async_remote_copy(
            src_ref=src,
            dst_ref=self.recvs[step].at[half],
            send_sem=self.send_sem.at[self.chunk, half, step],
            recv_sem=self.recv_sem.at[self.chunk, half, step],
            device_id=partners[step],
            device_id_type=MESH,
        )

    def start(self):
        for half in range(2):
            self.copy(half, 0).start()

    def advance(self):
        step = self.step
        if step >= STEPS:
            return
        for half in range(2):
            self.copy(half, step).wait()
            bits = self.where[half][0]
            at = (half, *bits[: step + 1])
            self.grad[at] = self.grad[at] + self.recvs[step][half]
            if step + 1 < STEPS:
                self.copy(half, step + 1).start()
        self.step += 1


def kernel(dims, *refs):
    win, count, dim, heads, entries, remote = dims
    width = dim // heads
    groups = heads // GROUP
    scale = width**-0.5
    tok, cot, reg, rel, w_qkv, w_proj, table = refs[:7]
    rest = refs[7:]
    if remote:
        out, out_table = rest[:2]
        rest = rest[2:]
    else:
        out_qkv, out_proj, out_table = rest[:3]
        rest = rest[3:]
    x, xt, c, qkv, d_att, att, d_qkv, probs, masks, bias, bias_rows, d_bias, small, rel_t, tab = rest[:15]
    rest = rest[15:]
    if remote:
        tab_buf, tab_recv, tab_send, tab_sem, send_sem, recv_sem, grad_p, grad_q = rest[:8]
        recv_p, recv_q = rest[8 : 8 + STEPS], rest[8 + STEPS : 8 + 2 * STEPS]
        gx, gy, gz = (lax.axis_index(a) for a in AXES)
        core, ypos, z0, z1 = gz % 2, gz // 2, gy % 2, gy // 2
        to_core = (gx, gy, gz + 1 - 2 * core)
        to_x = (1 - gx, gy, gz)
        to_y = (gx, gy, gz + 2 - 4 * ypos)
        to_z0 = (gx, gy + 1 - 2 * z0, gz)
        to_z1 = (gx, gy + 2 - 4 * z1, gz)
        where = (
            ((core, gx, ypos, z0, z1), (to_core, to_x, to_y, to_z0, to_z1)),
            ((core, ypos, gx, z0, z1), (to_core, to_y, to_x, to_z0, to_z1)),
        )
        barrier = pltpu.get_barrier_semaphore()
        for there in where[0][1]:
            pl.semaphore_signal(barrier, inc=1, device_id=there, device_id_type=MESH)
        pl.semaphore_wait(barrier, STEPS)

    lanes = lax.broadcasted_iota(jnp.int32, (PAD, GROUP * width), 1)

    x[...] = jnp.zeros_like(x)
    c[...] = jnp.zeros_like(c)
    for w in range(win):
        x[pl.ds(w * PAD, count), :] = tok[w]
        c[pl.ds(w * PAD, count), :] = cot[w]
    rows_all = win * PAD

    @pl.loop(0, rows_all // 256)
    def _(i):
        rows = pl.ds(pl.multiple_of(i * 256, 256), 256)
        qkv[rows, :] = dot(x[rows, :], w_qkv[...]).astype(BF16)
        d_att[rows, :] = dot(c[rows, :], w_proj[...], NT).astype(BF16)

    xt[...] = x[...].T

    small[...] = jnp.zeros_like(small)
    small[0:win, 0:count] = reg[...].astype(F32)
    reg_rows = small[...]
    reg_cols = reg_rows.T
    for w in range(win):
        row = reg_rows[w : w + 1, :PAD]
        row = jnp.concatenate([row, row], axis=1)
        masks[w * PAD : (w + 1) * PAD, :] = jnp.where(
            reg_cols[:PAD, w : w + 1] == row, 0.0, -100.0 * LOG2E
        )

    small[...] = jnp.full_like(small, -1.0)
    small[0:count, 0:count] = rel[...].astype(F32)
    rel_t[...] = small[...].T
    tab[...] = jnp.zeros_like(tab)
    tab[0:entries, 0:heads] = table[...]
    size = tab.shape[0]
    tab_t = tab[...].T[:heads]
    high = tab_t.astype(BF16)
    low = (tab_t - high.astype(F32)).astype(BF16)
    both = jnp.concatenate([high, low], axis=0)
    entry = lax.broadcasted_iota(jnp.int32, (size, 128), 0).astype(F32)

    def one_hot(j):
        return jnp.where(entry == rel_t[pl.ds(j, 1), :], 1.0, 0.0).astype(BF16)

    bias_rows[...] = jnp.full_like(bias_rows, -1e30)

    def look(j, carry):
        found = dot(both, one_hot(j))
        bias_rows[pl.ds(pl.multiple_of(j * heads, heads), heads), :] = (
            found[:heads] + found[heads:]
        ) * LOG2E
        return carry

    lax.fori_loop(0, count, look, 0)
    for g in range(groups):
        bias[g] = jnp.concatenate(
            [bias_rows[pl.ds(g * GROUP + h, PAD, stride=heads), :][:, :PAD] for h in range(GROUP)],
            axis=1,
        )
    d_bias[...] = jnp.zeros_like(d_bias)

    def rows_of(w):
        return pl.ds(pl.multiple_of(w * PAD, PAD), PAD)

    def part(ref, which, g, rows):
        at = which * dim + g * GROUP * width
        return ref[rows, at : at + GROUP * width]

    def forward(w, carry):
        rows = rows_of(w)
        mask = masks[rows, :]
        mask = jnp.concatenate([mask] * (GROUP * PAD // 128), axis=1)
        for g in range(groups):
            queries = spread(part(qkv, 0, g, rows), lanes, width)
            scores = dot(part(qkv, 1, g, rows), queries, NT)
            scores = scores * (scale * LOG2E) + bias[g] + mask
            raised = jnp.exp2(scores - jnp.max(scores, axis=0, keepdims=True))
            p = (raised * (1.0 / jnp.sum(raised, axis=0, keepdims=True))).astype(BF16)
            probs[g, rows, :] = p
            mixed = dot(p, part(qkv, 2, g, rows), TN)
            at = g * GROUP * width
            att[rows, at : at + GROUP * width] = gather_heads(mixed, lanes, width).astype(BF16)
        return carry

    lax.fori_loop(0, win, forward, 0)

    def place(value, ref):
        for d in range(value.shape[0] // 16):
            dx, dy, dz = d // 16, (d // 4) % 4, d % 4
            for half in range(2):
                a, b = (dx, dz // 2) if half == 0 else (dz // 2, dx)
                block = value[16 * d + 8 * half : 16 * d + 8 * half + 8]
                ref[half, dz % 2, a, b, dy % 2, dy // 2] = block

    g_proj = dot(att[...], c[...], TN)
    active = []
    if remote:
        place(g_proj, grad_p)
        active.append(Exchange(grad_p, recv_p, send_sem, recv_sem, 0, where))
        active[0].start()
    else:
        out_proj[...] = g_proj

    def backward(g):
        def one(w, carry):
            rows = rows_of(w)
            queries = spread(part(qkv, 0, g, rows), lanes, width)
            d_out = spread(part(d_att, 0, g, rows), lanes, width)
            p = probs[g, rows, :]
            d_probs = dot(part(qkv, 2, g, rows), d_out, NT)
            pf = p.astype(F32)
            weighted = pf * d_probs
            d_scores = weighted - pf * jnp.sum(weighted, axis=0, keepdims=True)
            d_bias[g] += d_scores
            ds = d_scores.astype(BF16)
            d_v = dot(p, d_out)
            d_k = dot(ds, queries) * scale
            d_q = gather_heads(dot(ds, part(qkv, 1, g, rows), TN), lanes, width) * scale
            d_qkv[rows, :] = jnp.concatenate([d_q, d_k, d_v], axis=1).astype(BF16)
            return carry

        return one

    pieces = 4
    wide = GROUP * width
    for g in range(groups):
        for s in range(pieces):
            lax.fori_loop(s * win // pieces, (s + 1) * win // pieces, backward(g), 0, unroll=2)
            for each in active:
                each.advance()
        g_qkv = dot(xt[...], d_qkv[...])
        if remote:
            place(g_qkv, grad_q.at[g])
            active.append(Exchange(grad_q.at[g], [r.at[g] for r in recv_q], send_sem, recv_sem, g + 1, where))
            active[-1].start()
        else:
            for which in range(3):
                at = which * dim + g * wide
                out_qkv[:, at : at + wide] = g_qkv[:, which * wide : (which + 1) * wide]

    for each in active:
        each.advance()

    for g in range(groups):
        for h in range(GROUP):
            piece = d_bias[g, :, h * PAD : (h + 1) * PAD]
            bias_rows[pl.ds(g * GROUP + h, PAD, stride=heads), :] = jnp.concatenate(
                [piece, jnp.zeros_like(piece)], axis=1
            )

    def collect(j, total):
        value = bias_rows[pl.ds(pl.multiple_of(j * heads, heads), heads), :]
        top = value.astype(BF16)
        rest_of = (value - top.astype(F32)).astype(BF16)
        return total + dot(jnp.concatenate([top, rest_of], axis=0), one_hot(j), NT)

    g_table = lax.fori_loop(0, count, collect, jnp.zeros((2 * heads, size), F32))
    g_table = g_table[:heads] + g_table[heads:]
    if not remote:
        out_table[...] = g_table
        return

    tab_buf[0] = g_table
    for step in range(STEPS):
        sent = pltpu.make_async_remote_copy(
            src_ref=tab_buf.at[step],
            dst_ref=tab_recv.at[step],
            send_sem=tab_send.at[step],
            recv_sem=tab_sem.at[step],
            device_id=where[0][1][step],
            device_id_type=MESH,
        )
        sent.start()
        for each in active:
            each.advance()
        sent.wait()
        tab_buf[step + 1] = tab_buf[step] + tab_recv[step]
    for each in active:
        while each.step < STEPS:
            each.advance()
    out_table[...] = tab_buf[STEPS]
    for half in range(2):
        bits = where[half][0]
        rows = pl.ds(8 * half, 8)
        out[rows, 3 * dim :] = grad_p[(half, *bits)]
        for g in range(groups):
            done = grad_q[(g, half, *bits)]
            for which in range(3):
                at = which * dim + g * wide
                out[rows, at : at + wide] = done[:, which * wide : (which + 1) * wide]


def local_grads(remote, tokens, cotangent, regions, rel_index, w_qkv, w_proj, bias_table):
    win, count, dim = tokens.shape
    entries, heads = bias_table.shape
    groups = heads // GROUP
    rows = win * PAD
    wide = GROUP * (dim // heads)
    size = -(-entries // 128) * 128
    scratch = [
        pltpu.VMEM((rows, dim), BF16),
        pltpu.VMEM((dim, rows), BF16),
        pltpu.VMEM((rows, dim), BF16),
        pltpu.VMEM((rows, 3 * dim), BF16),
        pltpu.VMEM((rows, dim), BF16),
        pltpu.VMEM((rows, dim), BF16),
        pltpu.VMEM((rows, 3 * wide), BF16),
        pltpu.VMEM((groups, rows, GROUP * PAD), BF16),
        pltpu.VMEM((rows, 128), F32),
        pltpu.VMEM((groups, PAD, GROUP * PAD), F32),
        pltpu.VMEM((PAD * heads, 128), F32),
        pltpu.VMEM((groups, PAD, GROUP * PAD), F32),
        pltpu.VMEM((128, 128), F32),
        pltpu.VMEM((128, 128), F32),
        pltpu.VMEM((size, 128), F32),
    ]
    if remote:
        outs = ((dim // lax.axis_size(AXES), 4 * dim), (heads, size))
        scratch += [
            pltpu.VMEM((STEPS + 1, heads, size), F32),
            pltpu.VMEM((STEPS, heads, size), F32),
            pltpu.SemaphoreType.DMA((STEPS,)),
            pltpu.SemaphoreType.DMA((STEPS,)),
            pltpu.SemaphoreType.DMA((groups + 1, 2, STEPS)),
            pltpu.SemaphoreType.DMA((groups + 1, 2, STEPS)),
            pltpu.VMEM((2,) + (2,) * STEPS + (8, dim), F32),
            pltpu.VMEM((groups, 2) + (2,) * STEPS + (8, 3 * wide), F32),
        ]
        for step in range(STEPS):
            scratch.append(pltpu.VMEM((2,) + (2,) * (STEPS - 1 - step) + (8, dim), F32))
        for step in range(STEPS):
            scratch.append(
                pltpu.VMEM((groups, 2) + (2,) * (STEPS - 1 - step) + (8, 3 * wide), F32)
            )
        params = dict(collective_id=0, has_side_effects=True)
    else:
        outs = ((dim, 3 * dim), (dim, dim), (heads, size))
        params = dict()
    dims = (win, count, dim, heads, entries, remote)
    vmem = pl.BlockSpec(memory_space=pltpu.VMEM)
    return pl.pallas_call(
        functools.partial(kernel, dims),
        out_shape=[jax.ShapeDtypeStruct(o, F32) for o in outs],
        in_specs=[vmem] * 7,
        out_specs=[vmem] * len(outs),
        scratch_shapes=scratch,
        compiler_params=pltpu.CompilerParams(vmem_limit_bytes=60 * 1024 * 1024, **params),
    )(tokens, cotangent, regions, rel_index, w_qkv, w_proj, bias_table)


def body(
    tokens, cotangent, regions, rel_index, w_qkv, w_proj, bias_table, mom_qkv, mom_proj, mom_table
):
    dim = tokens.shape[2]
    entries = bias_table.shape[0]
    devices = lax.axis_size(AXES)
    sizes = tuple(lax.axis_size(a) for a in AXES)
    scale = 1.0 / (tokens.shape[0] * devices)
    args = (tokens, cotangent, regions, rel_index, w_qkv, w_proj, bias_table)
    if sizes == (2, 4, 4) and dim == 16 * devices:
        mine, table = local_grads(True, *args)
        qkv_mine, proj_mine = mine[:, : 3 * dim].reshape(-1), mine[:, 3 * dim :].reshape(-1)
    else:
        qkv, proj, table = local_grads(False, *args)
        qkv_mine = lax.psum_scatter(qkv.reshape(-1), AXES, tiled=True)
        proj_mine = lax.psum_scatter(proj.reshape(-1), AXES, tiled=True)
        table = lax.psum(table, AXES)
    return (
        0.9 * mom_qkv + qkv_mine * scale,
        0.9 * mom_proj + proj_mine * scale,
        0.9 * mom_table + table[:, :entries].T * scale,
    )


def solution(mesh):
    return jax.shard_map(
        body,
        mesh=mesh,
        in_specs=(
            P(AXES, None, None),
            P(AXES, None, None),
            P(AXES, None),
            P(),
            P(),
            P(),
            P(),
            P(AXES),
            P(AXES),
            P(),
        ),
        out_specs=(P(AXES), P(AXES), P()),
        check_vma=False,
    )
```

```python
import functools
import math

import jax
import jax.numpy as jnp
from jax import lax
from jax.experimental import pallas as pl
from jax.experimental.pallas import tpu as pltpu
from jax.sharding import PartitionSpec as P

AXES = ("gx", "gy", "gz")
MESH = pl.DeviceIdType.MESH
F32, BF16 = jnp.float32, jnp.bfloat16
PAD = 64
GROUP = 4
LOG2E = math.log2(math.e)
STEPS = 5
NT = (((1,), (1,)), ((), ()))
TN = (((0,), (0,)), ((), ()))


def dot(a, b, dims=(((1,), (0,)), ((), ()))):
    return lax.dot_general(a, b, dims, preferred_element_type=F32)


def spread(value, lanes, width):
    return jnp.concatenate(
        [jnp.where(lanes // width == h, value, jnp.zeros_like(value)) for h in range(GROUP)], axis=0
    )


def gather_heads(value, lanes, width):
    total = jnp.where(lanes // width == 0, value[:PAD], 0.0)
    for h in range(1, GROUP):
        total = jnp.where(lanes // width == h, value[h * PAD : (h + 1) * PAD], total)
    return total


class Exchange:
    def __init__(self, grad, recvs, send_sem, recv_sem, chunk, where):
        self.grad, self.recvs, self.send_sem, self.recv_sem = grad, recvs, send_sem, recv_sem
        self.chunk, self.where, self.step = chunk, where, 0

    def copy(self, half, step):
        bits, partners = self.where[half]
        src = self.grad.at[(half, *bits[:step], 1 - bits[step])]
        return pltpu.make_async_remote_copy(
            src_ref=src,
            dst_ref=self.recvs[step].at[half],
            send_sem=self.send_sem.at[self.chunk, half, step],
            recv_sem=self.recv_sem.at[self.chunk, half, step],
            device_id=partners[step],
            device_id_type=MESH,
        )

    def start(self):
        for half in range(2):
            self.copy(half, 0).start()

    def advance(self):
        step = self.step
        if step >= STEPS:
            return
        for half in range(2):
            self.copy(half, step).wait()
            bits = self.where[half][0]
            at = (half, *bits[: step + 1])
            self.grad[at] = self.grad[at] + self.recvs[step][half]
            if step + 1 < STEPS:
                self.copy(half, step + 1).start()
        self.step += 1


def kernel(dims, *refs):
    win, count, dim, heads, entries, remote = dims
    width = dim // heads
    groups = heads // GROUP
    scale = width**-0.5
    tok, cot, reg, rel, w_qkv, w_proj, table = refs[:7]
    rest = refs[7:]
    if remote:
        out, out_table = rest[:2]
        rest = rest[2:]
    else:
        out_qkv, out_proj, out_table = rest[:3]
        rest = rest[3:]
    x, xt, c, qkv, d_att, att, d_qkv, probs, masks, bias, bias_rows, d_bias, small, rel_t, tab = rest[:15]
    rest = rest[15:]
    if remote:
        tab_buf, tab_recv, tab_send, tab_sem, send_sem, recv_sem, grad_p, grad_q = rest[:8]
        recv_p, recv_q = rest[8 : 8 + STEPS], rest[8 + STEPS : 8 + 2 * STEPS]
        gx, gy, gz = (lax.axis_index(a) for a in AXES)
        core, ypos, z0, z1 = gz % 2, gz // 2, gy % 2, gy // 2
        to_core = (gx, gy, gz + 1 - 2 * core)
        to_x = (1 - gx, gy, gz)
        to_y = (gx, gy, gz + 2 - 4 * ypos)
        to_z0 = (gx, gy + 1 - 2 * z0, gz)
        to_z1 = (gx, gy + 2 - 4 * z1, gz)
        where = (
            ((core, gx, ypos, z0, z1), (to_core, to_x, to_y, to_z0, to_z1)),
            ((core, ypos, gx, z0, z1), (to_core, to_y, to_x, to_z0, to_z1)),
        )
        barrier = pltpu.get_barrier_semaphore()
        for there in where[0][1]:
            pl.semaphore_signal(barrier, inc=1, device_id=there, device_id_type=MESH)
        pl.semaphore_wait(barrier, STEPS)

    lanes = lax.broadcasted_iota(jnp.int32, (PAD, GROUP * width), 1)

    x[...] = jnp.zeros_like(x)
    c[...] = jnp.zeros_like(c)
    for w in range(win):
        x[pl.ds(w * PAD, count), :] = tok[w]
        c[pl.ds(w * PAD, count), :] = cot[w]
    rows_all = win * PAD

    @pl.loop(0, rows_all // 256)
    def _(i):
        rows = pl.ds(pl.multiple_of(i * 256, 256), 256)
        qkv[rows, :] = dot(x[rows, :], w_qkv[...]).astype(BF16)
        d_att[rows, :] = dot(c[rows, :], w_proj[...], NT).astype(BF16)

    xt[...] = x[...].T

    small[...] = jnp.zeros_like(small)
    small[0:win, 0:count] = reg[...].astype(F32)
    reg_rows = small[...]
    reg_cols = reg_rows.T
    for w in range(win):
        row = reg_rows[w : w + 1, :PAD]
        row = jnp.concatenate([row, row], axis=1)
        masks[w * PAD : (w + 1) * PAD, :] = jnp.where(
            reg_cols[:PAD, w : w + 1] == row, 0.0, -100.0 * LOG2E
        )

    small[...] = jnp.full_like(small, -1.0)
    small[0:count, 0:count] = rel[...].astype(F32)
    rel_t[...] = small[...].T
    tab[...] = jnp.zeros_like(tab)
    tab[0:entries, 0:heads] = table[...]
    size = tab.shape[0]
    tab_t = tab[...].T[:heads]
    high = tab_t.astype(BF16)
    low = (tab_t - high.astype(F32)).astype(BF16)
    both = jnp.concatenate([high, low], axis=0)
    entry = lax.broadcasted_iota(jnp.int32, (size, 128), 0).astype(F32)

    def one_hot(j):
        return jnp.where(entry == rel_t[pl.ds(j, 1), :], 1.0, 0.0).astype(BF16)

    bias_rows[...] = jnp.full_like(bias_rows, -1e30)

    def look(j, carry):
        found = dot(both, one_hot(j))
        bias_rows[pl.ds(pl.multiple_of(j * heads, heads), heads), :] = (
            found[:heads] + found[heads:]
        ) * LOG2E
        return carry

    lax.fori_loop(0, count, look, 0)
    for g in range(groups):
        bias[g] = jnp.concatenate(
            [bias_rows[pl.ds(g * GROUP + h, PAD, stride=heads), :][:, :PAD] for h in range(GROUP)],
            axis=1,
        )
    d_bias[...] = jnp.zeros_like(d_bias)

    def rows_of(w):
        at = w * PAD
        return pl.ds(at if isinstance(at, int) else pl.multiple_of(at, PAD), PAD)

    def part(ref, which, g, rows):
        at = which * dim + g * GROUP * width
        return ref[rows, at : at + GROUP * width]

    def forward(w, carry):
        rows = rows_of(w)
        mask = masks[rows, :]
        mask = jnp.concatenate([mask] * (GROUP * PAD // 128), axis=1)
        every = range(groups)
        queries = [spread(part(qkv, 0, g, rows), lanes, width) for g in every]
        scores = [dot(part(qkv, 1, g, rows), queries[g], NT) for g in every]
        scores = [scores[g] * (scale * LOG2E) + bias[g] + mask for g in every]
        raised = [jnp.exp2(v - jnp.max(v, axis=0, keepdims=True)) for v in scores]
        p = [(v * (1.0 / jnp.sum(v, axis=0, keepdims=True))).astype(BF16) for v in raised]
        mixed = [dot(p[g], part(qkv, 2, g, rows), TN) for g in every]
        joined = [gather_heads(v, lanes, width).astype(BF16) for v in mixed]
        att[rows, :] = jnp.concatenate(joined, axis=1)
        for g in every:
            probs[g, rows, :] = p[g]
        return carry

    lax.fori_loop(0, win, forward, 0)

    def place(value, ref):
        for d in range(value.shape[0] // 16):
            dx, dy, dz = d // 16, (d // 4) % 4, d % 4
            for half in range(2):
                a, b = (dx, dz // 2) if half == 0 else (dz // 2, dx)
                block = value[16 * d + 8 * half : 16 * d + 8 * half + 8]
                ref[half, dz % 2, a, b, dy % 2, dy // 2] = block

    g_proj = dot(att[...], c[...], TN)
    active = []
    if remote:
        place(g_proj, grad_p)
        active.append(Exchange(grad_p, recv_p, send_sem, recv_sem, 0, where))
        active[0].start()
    else:
        out_proj[...] = g_proj

    def backward(g, windows):
        rows = [rows_of(w) for w in windows]
        queries = [spread(part(qkv, 0, g, r), lanes, width) for r in rows]
        d_out = [spread(part(d_att, 0, g, r), lanes, width) for r in rows]
        p = [probs[g, r, :] for r in rows]
        every = range(len(rows))
        d_probs = [dot(part(qkv, 2, g, rows[n]), d_out[n], NT) for n in every]
        d_v = [dot(p[n], d_out[n]) for n in every]
        pf = [v.astype(F32) for v in p]
        weighted = [pf[n] * d_probs[n] for n in every]
        d_scores = [
            weighted[n] - pf[n] * jnp.sum(weighted[n], axis=0, keepdims=True) for n in every
        ]
        d_bias[g] += sum(d_scores[1:], d_scores[0])
        ds = [v.astype(BF16) for v in d_scores]
        d_k = [dot(ds[n], queries[n]) * scale for n in every]
        d_q = [dot(ds[n], part(qkv, 1, g, rows[n]), TN) for n in every]
        d_q = [gather_heads(v, lanes, width) * scale for v in d_q]
        for n in every:
            d_qkv[rows[n], :] = jnp.concatenate([d_q[n], d_k[n], d_v[n]], axis=1).astype(BF16)

    pieces = 4
    wide = GROUP * width
    for g in range(groups):
        for s in range(pieces):
            backward(g, range(s * win // pieces, (s + 1) * win // pieces))
            for each in active:
                each.advance()
        g_qkv = dot(xt[...], d_qkv[...])
        if remote:
            place(g_qkv, grad_q.at[g])
            active.append(Exchange(grad_q.at[g], [r.at[g] for r in recv_q], send_sem, recv_sem, g + 1, where))
            active[-1].start()
        else:
            for which in range(3):
                at = which * dim + g * wide
                out_qkv[:, at : at + wide] = g_qkv[:, which * wide : (which + 1) * wide]

    for each in active:
        each.advance()

    for g in range(groups):
        for h in range(GROUP):
            piece = d_bias[g, :, h * PAD : (h + 1) * PAD]
            bias_rows[pl.ds(g * GROUP + h, PAD, stride=heads), :] = jnp.concatenate(
                [piece, jnp.zeros_like(piece)], axis=1
            )

    def collect(j, total):
        value = bias_rows[pl.ds(pl.multiple_of(j * heads, heads), heads), :]
        top = value.astype(BF16)
        rest_of = (value - top.astype(F32)).astype(BF16)
        return total + dot(jnp.concatenate([top, rest_of], axis=0), one_hot(j), NT)

    g_table = lax.fori_loop(0, count, collect, jnp.zeros((2 * heads, size), F32))
    g_table = g_table[:heads] + g_table[heads:]
    if not remote:
        out_table[...] = g_table
        return

    tab_buf[0] = g_table
    for step in range(STEPS):
        sent = pltpu.make_async_remote_copy(
            src_ref=tab_buf.at[step],
            dst_ref=tab_recv.at[step],
            send_sem=tab_send.at[step],
            recv_sem=tab_sem.at[step],
            device_id=where[0][1][step],
            device_id_type=MESH,
        )
        sent.start()
        for each in active:
            each.advance()
        sent.wait()
        tab_buf[step + 1] = tab_buf[step] + tab_recv[step]
    for each in active:
        while each.step < STEPS:
            each.advance()
    out_table[...] = tab_buf[STEPS]
    for half in range(2):
        bits = where[half][0]
        rows = pl.ds(8 * half, 8)
        out[rows, 3 * dim :] = grad_p[(half, *bits)]
        for g in range(groups):
            done = grad_q[(g, half, *bits)]
            for which in range(3):
                at = which * dim + g * wide
                out[rows, at : at + wide] = done[:, which * wide : (which + 1) * wide]


def local_grads(remote, tokens, cotangent, regions, rel_index, w_qkv, w_proj, bias_table):
    win, count, dim = tokens.shape
    entries, heads = bias_table.shape
    groups = heads // GROUP
    rows = win * PAD
    wide = GROUP * (dim // heads)
    size = -(-entries // 128) * 128
    scratch = [
        pltpu.VMEM((rows, dim), BF16),
        pltpu.VMEM((dim, rows), BF16),
        pltpu.VMEM((rows, dim), BF16),
        pltpu.VMEM((rows, 3 * dim), BF16),
        pltpu.VMEM((rows, dim), BF16),
        pltpu.VMEM((rows, dim), BF16),
        pltpu.VMEM((rows, 3 * wide), BF16),
        pltpu.VMEM((groups, rows, GROUP * PAD), BF16),
        pltpu.VMEM((rows, 128), F32),
        pltpu.VMEM((groups, PAD, GROUP * PAD), F32),
        pltpu.VMEM((PAD * heads, 128), F32),
        pltpu.VMEM((groups, PAD, GROUP * PAD), F32),
        pltpu.VMEM((128, 128), F32),
        pltpu.VMEM((128, 128), F32),
        pltpu.VMEM((size, 128), F32),
    ]
    if remote:
        outs = ((dim // lax.axis_size(AXES), 4 * dim), (heads, size))
        scratch += [
            pltpu.VMEM((STEPS + 1, heads, size), F32),
            pltpu.VMEM((STEPS, heads, size), F32),
            pltpu.SemaphoreType.DMA((STEPS,)),
            pltpu.SemaphoreType.DMA((STEPS,)),
            pltpu.SemaphoreType.DMA((groups + 1, 2, STEPS)),
            pltpu.SemaphoreType.DMA((groups + 1, 2, STEPS)),
            pltpu.VMEM((2,) + (2,) * STEPS + (8, dim), F32),
            pltpu.VMEM((groups, 2) + (2,) * STEPS + (8, 3 * wide), F32),
        ]
        for step in range(STEPS):
            scratch.append(pltpu.VMEM((2,) + (2,) * (STEPS - 1 - step) + (8, dim), F32))
        for step in range(STEPS):
            scratch.append(
                pltpu.VMEM((groups, 2) + (2,) * (STEPS - 1 - step) + (8, 3 * wide), F32)
            )
        params = dict(collective_id=0, has_side_effects=True)
    else:
        outs = ((dim, 3 * dim), (dim, dim), (heads, size))
        params = dict()
    dims = (win, count, dim, heads, entries, remote)
    vmem = pl.BlockSpec(memory_space=pltpu.VMEM)
    return pl.pallas_call(
        functools.partial(kernel, dims),
        out_shape=[jax.ShapeDtypeStruct(o, F32) for o in outs],
        in_specs=[vmem] * 7,
        out_specs=[vmem] * len(outs),
        scratch_shapes=scratch,
        compiler_params=pltpu.CompilerParams(vmem_limit_bytes=60 * 1024 * 1024, **params),
    )(tokens, cotangent, regions, rel_index, w_qkv, w_proj, bias_table)


def body(
    tokens, cotangent, regions, rel_index, w_qkv, w_proj, bias_table, mom_qkv, mom_proj, mom_table
):
    dim = tokens.shape[2]
    entries = bias_table.shape[0]
    devices = lax.axis_size(AXES)
    sizes = tuple(lax.axis_size(a) for a in AXES)
    scale = 1.0 / (tokens.shape[0] * devices)
    args = (tokens, cotangent, regions, rel_index, w_qkv, w_proj, bias_table)
    if sizes == (2, 4, 4) and dim == 16 * devices:
        mine, table = local_grads(True, *args)
        qkv_mine, proj_mine = mine[:, : 3 * dim].reshape(-1), mine[:, 3 * dim :].reshape(-1)
    else:
        qkv, proj, table = local_grads(False, *args)
        qkv_mine = lax.psum_scatter(qkv.reshape(-1), AXES, tiled=True)
        proj_mine = lax.psum_scatter(proj.reshape(-1), AXES, tiled=True)
        table = lax.psum(table, AXES)
    return (
        0.9 * mom_qkv + qkv_mine * scale,
        0.9 * mom_proj + proj_mine * scale,
        0.9 * mom_table + table[:, :entries].T * scale,
    )


def solution(mesh):
    return jax.shard_map(
        body,
        mesh=mesh,
        in_specs=(
            P(AXES, None, None),
            P(AXES, None, None),
            P(AXES, None),
            P(),
            P(),
            P(),
            P(),
            P(AXES),
            P(AXES),
            P(),
        ),
        out_specs=(P(AXES), P(AXES), P()),
        check_vma=False,
    )
```
